256 devices in a mesh: dp: 32 (over x, z), mp: 8 (over y, core).
Axes of the slice: x: 4, y: 4, z: 8, core: 2. Of those that a mesh axis runs over, the one named last changes fastest.
Arguments:
- query_emb: bfloat16 [8192, 768], P('dp'), may hold values from -6 to 6
- positive_list: int32 [8192], replicated, may hold values from 0 to 32767
- centroids: float32 [32768, 768], P(('dp', 'mp')), may hold values from -0.6 to 0.6
- first_moment: float32 [32768, 768], P(('dp', 'mp')), may hold values from -3 to 3
- second_moment: float32 [32768, 768], P(('dp', 'mp')), may hold values from 0.05 to 2
Outputs:
- new_centroids: float32 [32768, 768], P(('dp', 'mp'))
- new_first: float32 [32768, 768], P(('dp', 'mp'))
- new_second: float32 [32768, 768], P(('dp', 'mp'))
- mean_loss: float32 [], replicated
The draws below stay inside these ranges and needn't reach their ends.
All inputs are finite; a program needn't handle non-finite values.
Results may differ from the reference program's by a relative error of at most 0.00097.
Values may be sent and summed in bfloat16 or wider, within the bound.
No kernel may reach another device: no remote copies, remote signals or barrier semaphores. Data moves between devices by JAX's collectives and lax.ppermute only.
A program may use at most 64 MiB of HBM per device.

```python
import math
import jax
import jax.numpy as jnp
from jax import lax

D = 768
LISTS = 32768
ROWS = 8192


def centroid_rows(key):
    base_scale = 3.5 / math.sqrt(D)
    base = jnp.clip(base_scale * jax.random.normal(key, (LISTS, D), jnp.float32), -0.6, 0.6)
    signs = jnp.where(jax.random.normal(jax.random.fold_in(key, 3), (LISTS, D), jnp.float32) >= 0.0, base_scale, -base_scale)
    list_ids = jnp.arange(LISTS, dtype=jnp.int32)
    peaked = (list_ids % 1024 == 5)[:, None]
    return jnp.where(peaked, signs, base)


def draw_centroids(key, part):
    return centroid_rows(jax.random.fold_in(key, 11))


def draw_query_emb(key, part):
    base_scale = 3.5 / math.sqrt(D)
    aligned_size = min(6.0, 290.0 / (base_scale * D))
    table_full = centroid_rows(jax.random.fold_in(key, 11))
    noise_key = jax.random.fold_in(key, 12)
    background = jnp.clip(jax.random.normal(noise_key, (ROWS, D), jnp.float32), -6.0, 6.0)
    row_ids = jnp.arange(ROWS, dtype=jnp.int32)
    picked = (row_ids // 64 * 1024 + 5) % LISTS
    aligned = aligned_size * jnp.sign(table_full[picked])
    chosen = (row_ids % 64 == 0)[:, None]
    values = jnp.where(chosen, aligned, background)
    return values.astype(jnp.bfloat16)


def set_ends(array, stream_key, least, top_value):
    place = [jax.random.randint(jax.random.fold_in(stream_key, axis), (), 0, length) for axis, length in enumerate(array.shape)]
    widest = array.shape.index(max(array.shape))
    neighbour = place[:widest] + [(place[widest] + 1) % array.shape[widest]] + place[widest + 1:]
    return array.at[tuple(place)].set(least).at[tuple(neighbour)].set(top_value)


def block_levels(rng, extent, shards, smallest, high):
    level, own = 1.0, jax.random.fold_in(rng, 6)
    for axis_at, blocks in shards:
        heights = jnp.exp(jax.random.uniform(jax.random.fold_in(own, axis_at), (blocks,), jnp.float32, smallest / len(shards), high / len(shards)))
        level = level * jnp.repeat(heights, extent[axis_at] // blocks).reshape([-1 if axis == axis_at else 1 for axis in range(len(extent))])
    return level


def normal_values(own_key, extent, width, bound, cuts=(), kind=jnp.bfloat16):
    drawn = width * jax.random.normal(own_key, extent, jnp.float32)
    if cuts:
        drawn = drawn * block_levels(own_key, extent, cuts, -0.22, 0.18)
    return jnp.clip(drawn, -bound, bound).astype(kind)


def setup_inputs(seed: int = 0) -> dict:
    key_of = jax.random.split(jax.random.key(seed), 6)
    query_emb = draw_query_emb(jax.random.fold_in(key_of[5], 71), 0)
    positive_list = set_ends(jax.random.randint(key_of[1], (ROWS,), 0, LISTS), jax.random.fold_in(key_of[1], 1), 0, LISTS - 1).astype(jnp.int32)
    centroids = draw_centroids(jax.random.fold_in(key_of[5], 71), 0)
    first_moment = normal_values(key_of[3], (LISTS, D), 0.5, 3.0, ((0, 256),), jnp.float32)
    second_moment = jnp.clip(jnp.exp(math.log(2.0) - 3.6888794 * jax.random.uniform(key_of[4], (LISTS, D), jnp.float32) ** block_levels(key_of[4], (LISTS, D), ((0, 256),), -0.2, 0.2)), 0.05, 2.0)
    return {"query_emb": query_emb, "positive_list": positive_list, "centroids": centroids, "first_moment": first_moment, "second_moment": second_moment}


beta_first = 0.9
beta_second = 0.95
learn_rate = 0.01
epsilon = 1e-08

def adam_update(centroids, first_moment, second_moment, gradient):
    new_first = beta_first * first_moment + (1.0 - beta_first) * gradient
    new_second = beta_second * second_moment + (1.0 - beta_second) * gradient * gradient
    new_centroids = centroids - learn_rate * new_first / (jnp.sqrt(new_second) + epsilon)
    return (new_centroids, new_first, new_second)

def reference(query_emb, positive_list, centroids, first_moment, second_moment):
    table_half = centroids.astype(jnp.bfloat16)
    block_rows = math.gcd(ROWS, 512)
    query_blocks = query_emb.reshape(ROWS // block_rows, block_rows, D)
    target_blocks = positive_list.reshape(ROWS // block_rows, block_rows)
    list_ids = jnp.arange(LISTS, dtype=jnp.int32)

    def scan_step(state_pair, block_item):
        gradient, loss_sum = state_pair
        queries, targets = block_item
        logits = jnp.dot(queries, table_half.T, preferred_element_type=jnp.float32)
        row_peak = lax.optimization_barrier(jnp.max(logits, axis=1))
        row_mass = lax.optimization_barrier(jnp.sum(jnp.exp(logits - row_peak[:, None]), axis=1))
        log_norm = row_peak + jnp.log(row_mass)
        is_target = list_ids[None, :] == targets[:, None].astype(jnp.int32)
        row_target = lax.optimization_barrier(jnp.sum(jnp.where(is_target, logits, jnp.zeros_like(logits)), axis=1))
        loss_sum = loss_sum + jnp.sum(log_norm - row_target)
        weights = (jnp.exp(logits - log_norm[:, None]) - is_target.astype(jnp.float32)).astype(jnp.bfloat16)
        gradient = gradient + jnp.dot(weights.T, queries, preferred_element_type=jnp.float32)
        return ((gradient, loss_sum), None)
    start_state = (jnp.zeros((LISTS, D), jnp.float32), jnp.zeros((), jnp.float32))
    final_state, unused = lax.scan(scan_step, start_state, (query_blocks, target_blocks))
    gradient, loss_sum = final_state
    new_centroids, new_first, new_second = adam_update(centroids, first_moment, second_moment, gradient)
    return (new_centroids, new_first, new_second, loss_sum / ROWS)
```

```python
import jax
import jax.numpy as jnp
from jax import lax
from jax.sharding import Mesh
from jax.sharding import PartitionSpec as P

MP = ("y", "c")
DP = ("x", "z")
DP_MP = ("x", "z", "y", "c")

beta_first = 0.9
beta_second = 0.95
learn_rate = 0.01
epsilon = 1e-08
ROWS = 8192
BLOCK = 256
HALF = 128


def turn(size, step):
    return [(i, (i + step) % size) for i in range(size)]


SWAP = [(0, 1), (1, 0)]
OPPOSITE = [(z * 2 + c, (z + (1, -1)[c]) % 8 * 2 + c) for z in range(8) for c in range(2)]


def adam_update(centroids, first_moment, second_moment, gradient):
    new_first = beta_first * first_moment + (1.0 - beta_first) * gradient
    new_second = beta_second * second_moment + (1.0 - beta_second) * gradient * gradient
    new_centroids = centroids - learn_rate * new_first / (jnp.sqrt(new_second) + epsilon)
    return (new_centroids, new_first, new_second)


def gather_lists(own):
    return [own] + [lax.ppermute(own, "x", turn(4, step)) for step in (1, -1, 2)]


def gather_rows(own, core):
    parts = [own[:HALF], own[HALF:]]
    mine, other = [], []
    for _ in range(3):
        parts = [lax.ppermute(part, ("z", "c"), OPPOSITE) for part in parts]
        mine.append(list(parts))
        other.append([lax.ppermute(part, "c", SWAP) for part in parts])
    last = lax.ppermute(jnp.where(core == 0, parts[0], parts[1]), ("z", "c"), OPPOSITE)
    swapped = lax.ppermute(last, "c", SWAP)
    far = [jnp.where(core == 0, last, swapped), jnp.where(core == 0, swapped, last)]
    return [own] + mine + other + [far]


def log_sum_exp(parts):
    top = jnp.max(parts, axis=0)
    joined = top + jnp.log(jnp.sum(jnp.exp(parts - top[None]), axis=0))
    row = lax.broadcasted_iota(jnp.int32, joined.shape, 0)
    return jnp.where(row < 16, joined, jnp.sum(parts, axis=0))


def shards(query_emb, positive_list, centroids, first_moment, second_moment):
    x, z, y, core = (lax.axis_index(name) for name in DP_MP)
    sign = 1 - 2 * core
    lists = jnp.concatenate(gather_lists(centroids.astype(jnp.bfloat16)))
    pieces = gather_rows(query_emb, core)
    rows = jnp.concatenate([part for piece in pieces for part in (piece if isinstance(piece, list) else [piece])])
    steps = jnp.stack([0 * sign] + [-sign * k for k in (1, 2, 3)] + [sign * k for k in (1, 2, 3)] + [4 * sign])
    block = (z + steps) % 8
    hops = jnp.array([0, -1, 1, 2], jnp.int32)
    list_block = ((x + hops) % 4 * 8 + z) * 8 + y * 2 + core
    list_ids = (list_block[:, None] * 128 + jnp.arange(128, dtype=jnp.int32)).reshape(-1)
    targets = positive_list.reshape(4, 8, BLOCK)[x][block].reshape(-1)

    logits = jnp.einsum("rd,kd->rk", rows, lists, preferred_element_type=jnp.float32)
    is_target = list_ids[None, :] == targets[:, None]
    peak = jnp.max(logits, axis=1)
    mass = jnp.sum(jnp.exp(logits - peak[:, None]), axis=1)
    hit = jnp.sum(jnp.where(is_target, logits, jnp.zeros_like(logits)))
    local = (peak + jnp.log(mass)).reshape(8, BLOCK)
    slot_of = jnp.argmax(block[None, :] == jnp.arange(8)[:, None], axis=1)
    local = local[slot_of].reshape(16, 128)
    state = jnp.concatenate([local, jnp.full((8, 128), hit / 1024.0)])
    state = log_sum_exp(jnp.stack([state, lax.ppermute(state, "c", SWAP)]))
    state = log_sum_exp(jnp.stack([state] + [lax.ppermute(state, "y", turn(4, step)) for step in (1, -1, 2)]))
    state = log_sum_exp(lax.all_to_all(jnp.broadcast_to(state[None], (8, 24, 128)), "z", 0, 0))
    log_norm = state[:16].reshape(8, BLOCK)
    loss = jnp.broadcast_to(jnp.sum(log_norm) - jnp.sum(state[16:]), (8, 128))
    log_norm = log_norm[block].reshape(-1)

    weights = (jnp.exp(logits - log_norm[:, None]) - is_target.astype(jnp.float32)).astype(jnp.bfloat16)
    gradient = jnp.einsum("rk,rd->kd", weights, rows, preferred_element_type=jnp.float32)
    parts = gradient.reshape(4, 128, -1)
    back = [lax.ppermute(part, "x", turn(4, step)) for part, step in ((parts[1], -1), (parts[2], 1))]
    half = 64
    ahead = lax.ppermute(parts[3, :half], "x", turn(4, 2))
    behind = lax.ppermute(parts[3, half:], "x", turn(4, -2))
    gradient = parts[0] + back[0] + back[1] + jnp.concatenate([ahead, behind])
    loss = loss + sum(lax.ppermute(loss, "x", turn(4, step)) for step in (1, -1, 2))
    new_centroids, new_first, new_second = adam_update(centroids, first_moment, second_moment, gradient)
    return (new_centroids, new_first, new_second, loss[0, 0] / ROWS)


def solution(mesh):
    split = Mesh(mesh.devices.reshape(4, 8, 4, 2), DP_MP)
    placed = (P(DP, None), P(), P(DP_MP, None), P(DP_MP, None), P(DP_MP, None))
    return jax.shard_map(
        shards,
        mesh=split,
        in_specs=placed,
        out_specs=(P(DP_MP, None), P(DP_MP, None), P(DP_MP, None), P()),
        check_vma=False,
    )
```

```python
import functools

import jax
import jax.numpy as jnp
from jax import lax
from jax.experimental import pallas as pl
from jax.experimental.pallas import tpu as pltpu
from jax.sharding import Mesh
from jax.sharding import PartitionSpec as P

DP = ("x", "z")
DP_MP = ("x", "z", "y", "c")

beta_first = 0.9
beta_second = 0.95
learn_rate = 0.01
epsilon = 1e-08
ROWS = 8192
WIDTH = 768
BLOCK = 256
HALF = 128
OWN = 128
HOPS = (0, 2, 1, 3)
LISTS = OWN * len(HOPS)
SCALE = 4.0


def turn(size, step):
    return [(i, (i + step) % size) for i in range(size)]


SWAP = [(0, 1), (1, 0)]
OPPOSITE = [(z * 2 + c, (z + (1, -1)[c]) % 8 * 2 + c) for z in range(8) for c in range(2)]
VMEM = pl.BlockSpec(memory_space=pltpu.VMEM)
SMEM = pl.BlockSpec(memory_space=pltpu.SMEM)


def adam_update(centroids, first_moment, second_moment, gradient):
    new_first = beta_first * first_moment + (1.0 - beta_first) * gradient
    new_second = beta_second * second_moment + (1.0 - beta_second) * gradient * gradient
    new_centroids = centroids - learn_rate * new_first / (jnp.sqrt(new_second) + epsilon)
    return (new_centroids, new_first, new_second)


def place_of(device):
    core = lax.rem(device, 2)
    return lax.div(device, 64), lax.rem(lax.div(device, 8), 8), lax.rem(device, 8), 1 - 2 * core


def source(z, sign, slot):
    step = 0 if slot == 0 else 4 if slot == 7 else -sign * slot if slot < 4 else sign * (slot - 3)
    return lax.rem(z + step + 8, 8)


def targets_of(positive_ref, x, z, sign, slots):
    return jnp.concatenate([positive_ref[pl.ds(x * 8 + source(z, sign, slot), 1), :] for slot in slots], axis=1)


def list_ids(x, z, rest, j, width):
    first = ((lax.rem(x + HOPS[j], 4) * 8 + z) * 8 + rest) * OWN
    return first + lax.broadcasted_iota(jnp.int32, (OWN, width), 0)


def forward_kernel(slots, n_rows, device_ref, positive_ref, *refs):
    lists = refs[: len(HOPS)]
    rows = refs[len(HOPS) : len(HOPS) + n_rows]
    power_ref, sums_ref = refs[-2:]
    x, z, rest, sign = place_of(device_ref[0])
    row = jnp.concatenate([ref[...] for ref in rows])
    width = row.shape[0]
    target = targets_of(positive_ref, x, z, sign, slots)
    logits, hit = [], jnp.zeros((1, width), jnp.float32)
    for j, ref in enumerate(lists):
        value = lax.dot_general(ref[...], row, (((1,), (1,)), ((), ())), preferred_element_type=jnp.float32)
        is_target = list_ids(x, z, rest, j, width) == target
        hit = hit + jnp.sum(jnp.where(is_target, value, 0.0), axis=0, keepdims=True)
        logits.append(value)
    peak = functools.reduce(jnp.maximum, [jnp.max(value, axis=0, keepdims=True) for value in logits])
    mass = jnp.zeros((1, width), jnp.float32)
    for j, value in enumerate(logits):
        power = jnp.exp(value - peak)
        power_ref[j * OWN : (j + 1) * OWN, :] = power
        mass = mass + jnp.sum(power, axis=0, keepdims=True)
    sums_ref[0:1, :] = peak + jnp.log(mass)
    sums_ref[1:2, :] = peak
    sums_ref[2:3, :] = hit


def forward(slots, device, positive, lists, rows):
    width = sum(row.shape[0] for row in rows)
    return pl.pallas_call(
        functools.partial(forward_kernel, slots, len(rows)),
        out_shape=(
            jax.ShapeDtypeStruct((LISTS, width), jnp.float32),
            jax.ShapeDtypeStruct((8, width), jnp.float32),
        ),
        in_specs=[SMEM] + [VMEM] * (1 + len(lists) + len(rows)),
        out_specs=(VMEM, VMEM),
        cost_estimate=pl.CostEstimate(
            flops=2 * width * LISTS * WIDTH,
            bytes_accessed=2 * WIDTH * (width + LISTS),
            transcendentals=width * LISTS,
        ),
        name="forward",
    )(device, positive, *lists, *rows)


SLOTS = ((0,), (1, 4), (2, 5), (3, 6), (7,))


def gather_state(device_ref, *refs):
    sums, state_ref = refs[:-1], refs[-1]
    x, z, rest, sign = place_of(device_ref[0])
    state_ref[:, BLOCK:] = jnp.zeros((8, 128), jnp.float32)
    hit = jnp.zeros((1, 128), jnp.float32)
    for slots, ref in zip(SLOTS, sums):
        for i, slot in enumerate(slots):
            at = i * BLOCK
            state_ref[pl.ds(source(z, sign, slot), 1), :BLOCK] = ref[0:1, at : at + BLOCK]
            hit = hit + ref[2:3, at : at + 128] + ref[2:3, at + 128 : at + BLOCK]
    state_ref[0:1, BLOCK:] = hit


def join(parts):
    top = jnp.max(parts, axis=0)
    joined = top + jnp.log(jnp.sum(jnp.exp(parts - top[None]), axis=0))
    return jnp.where(lax.broadcasted_iota(jnp.int32, top.shape, 1) < BLOCK, joined, jnp.sum(parts, axis=0))


def backward_kernel(blocks, device_ref, positive_ref, state_ref, *refs):
    powers, sums, rows = refs[:5], refs[5:10], refs[10:25]
    gradient_ref, loss_ref, norm_ref = refs[25:]
    x, z, rest, sign = place_of(device_ref[0])
    state = join(state_ref[...])
    norm_ref[...] = state
    lane = lax.broadcasted_iota(jnp.int32, state.shape, 1)
    loss_ref[...] = jnp.full((8, 128), jnp.sum(jnp.where(lane < BLOCK, state, -state)))
    at = 0
    for slots, power_ref, sums_ref in zip(SLOTS, powers, sums):
        for i, slot in enumerate(slots):
            count = 1 if slot == 0 else 2
            row = jnp.concatenate([ref[...] for ref in rows[at : at + count]])
            at += count
            lanes = slice(i * BLOCK, (i + 1) * BLOCK)
            factor = jnp.exp(sums_ref[1:2, lanes] - norm_ref[pl.ds(source(z, sign, slot), 1), :BLOCK])
            target = targets_of(positive_ref, x, z, sign, (slot,))
            weights = []
            for j in blocks:
                is_target = list_ids(x, z, rest, j, BLOCK) == target
                weight = power_ref[j * OWN : (j + 1) * OWN, lanes] * factor - is_target.astype(jnp.float32)
                weights.append(weight.astype(jnp.bfloat16))
            part = jnp.dot(jnp.concatenate(weights), row, preferred_element_type=jnp.float32)
            if slot == 0:
                gradient_ref[...] = part
            else:
                gradient_ref[...] += part


def backward(blocks, device, positive, state, powers, sums, rows):
    return pl.pallas_call(
        functools.partial(backward_kernel, blocks),
        out_shape=(
            jax.ShapeDtypeStruct((OWN * len(blocks), WIDTH), jnp.float32),
            jax.ShapeDtypeStruct((8, 128), jnp.float32),
        ),
        in_specs=[SMEM] + [VMEM] * (2 + len(powers) + len(sums) + len(rows)),
        out_specs=(VMEM, VMEM),
        scratch_shapes=[pltpu.VMEM((8, BLOCK + 128), jnp.float32)],
        cost_estimate=pl.CostEstimate(
            flops=2 * 2048 * OWN * len(blocks) * WIDTH, bytes_accessed=6 * 2048 * WIDTH, transcendentals=0
        ),
        name="backward",
    )(device, positive, state, *powers, *sums, *rows)


def shards(query_emb, positive_list, centroids, first_moment, second_moment):
    core = lax.axis_index("c")
    device = jnp.full((8,), lax.axis_index(DP_MP), jnp.int32)
    positive = positive_list.reshape(32, BLOCK)

    parts = [query_emb[:HALF], query_emb[HALF:]]
    mine, other = [], []
    for _ in range(3):
        parts = [lax.ppermute(part, ("z", "c"), OPPOSITE) for part in parts]
        mine.append(parts)
        other.append([lax.ppermute(part, "c", SWAP) for part in parts])
    last = lax.ppermute(jnp.where(core == 0, parts[0], parts[1]), ("z", "c"), OPPOSITE)
    swapped = lax.ppermute(last, "c", SWAP)
    far = [jnp.where(core == 0, last, swapped), jnp.where(core == 0, swapped, last)]
    rows = [[query_emb]] + [mine[k] + other[k] for k in range(3)] + [far]

    half = centroids.astype(jnp.bfloat16)
    lists = [half] + [lax.ppermute(half, "x", turn(4, -hop)) for hop in HOPS[1:]]

    done = [forward(slots, device, positive, lists, row) for slots, row in zip(SLOTS, rows)]
    powers, sums = [pair[0] for pair in done], [pair[1] for pair in done]
    state = pl.pallas_call(
        gather_state,
        out_shape=jax.ShapeDtypeStruct((8, BLOCK + 128), jnp.float32),
        in_specs=[SMEM] + [VMEM] * 5,
        out_specs=VMEM,
        name="state",
    )(device, *sums)
    state = join(jnp.stack([state, lax.ppermute(state, "c", SWAP)]))
    state = lax.all_to_all(jnp.broadcast_to(state[None], (32,) + state.shape), ("z", "y"), 0, 0)

    flat = [part for row in rows for part in row]
    first, loss = backward((1, 2), device, positive, state, powers, sums, flat)
    second, _ = backward((3, 0), device, positive, state, powers, sums, flat)
    sent = (first * SCALE).astype(jnp.float16)
    back = [
        lax.ppermute(sent[:64], "x", turn(4, 2)),
        lax.ppermute(sent[64:OWN], "x", turn(4, -2)),
        lax.ppermute(sent[OWN:], "x", turn(4, 1)),
        lax.ppermute((second[:OWN] * SCALE).astype(jnp.float16), "x", turn(4, -1)),
    ]
    back = [part.astype(jnp.float32) for part in back]
    gradient = second[OWN:] + (jnp.concatenate(back[:2]) + back[2] + back[3]) * (1.0 / SCALE)
    loss = loss + sum(lax.ppermute(loss, "x", turn(4, step)) for step in (1, -1, 2))
    new_centroids, new_first, new_second = adam_update(centroids, first_moment, second_moment, gradient)
    return (new_centroids, new_first, new_second, loss[0, 0] / ROWS)


def solution(mesh):
    split = Mesh(mesh.devices.reshape(4, 8, 4, 2), DP_MP)
    placed = (P(DP, None), P(), P(DP_MP, None), P(DP_MP, None), P(DP_MP, None))
    return jax.shard_map(
        shards,
        mesh=split,
        in_specs=placed,
        out_specs=(P(DP_MP, None), P(DP_MP, None), P(DP_MP, None), P()),
        check_vma=False,
    )
```

```python
import functools

import jax
import jax.numpy as jnp
import numpy as np
from jax import lax
from jax.sharding import Mesh
from jax.sharding import PartitionSpec as P


DP = ("x", "z")
DP_MP = ("x", "z", "y", "c")

beta_first = 0.9
beta_second = 0.95
learn_rate = 0.01
epsilon = 1e-08
ROWS = 8192
HALF = 128
OWN = 128
HOPS = (1, 2, 3, 0)
ZERO = np.uint32(0)
SCALE = 4.0


def turn(size, step):
    return [(i, (i + step) % size) for i in range(size)]


SWAP = [(0, 1), (1, 0)]
OPPOSITE = [(z * 2 + c, (z + (1, -1)[c]) % 8 * 2 + c) for z in range(8) for c in range(2)]


def adam_update(centroids, first_moment, second_moment, gradient):
    new_first = beta_first * first_moment + (1.0 - beta_first) * gradient
    new_second = beta_second * second_moment + (1.0 - beta_second) * gradient * gradient
    new_centroids = centroids - learn_rate * new_first / (jnp.sqrt(new_second) + epsilon)
    return (new_centroids, new_first, new_second)


def join(*parts):
    top = functools.reduce(jnp.maximum, parts)
    joined = top + jnp.log(sum(jnp.exp(part - top) for part in parts))
    return jnp.where(lax.broadcasted_iota(jnp.int32, top.shape, 0) < 16, joined, sum(parts))


def over_lists(state, at_first):
    state = join(state, lax.ppermute(state, "c", SWAP))
    pair = join(state, lax.ppermute(state, ("z", "c"), OPPOSITE))
    some = lax.ppermute(pair, ("z", "c"), [(z * 2 + c, (z + (2, -1)[c]) % 8 * 2 + c) for z in range(8) for c in range(2)])
    rest = lax.ppermute(pair, ("z", "c"), [(z * 2 + 1, (z - 3) % 8 * 2 + 1) for z in range(8)])
    state = join(some, jnp.where(at_first, pair, rest))
    state = join(state, *[lax.ppermute(state, "y", turn(4, step)) for step in (2, 1, -1)])
    return join(state, lax.ppermute(state, "c", SWAP))


def is_target(targets):
    return lax.broadcasted_iota(jnp.int32, (4 * OWN, targets.shape[0]), 0) == targets[None, :]


def logits_of(rows, lists):
    return jnp.einsum("kd,rd->kr", lists, rows, preferred_element_type=jnp.float32)


def logits_of(rows, lists):
    return jnp.einsum("kd,rd->kr", lists, rows, preferred_element_type=jnp.float32)


def forward(rows, lists, targets):
    logits = logits_of(rows, lists)
    peak = jnp.max(logits, axis=0)
    logits, peak = lax.optimization_barrier((logits, peak))
    total = jnp.sum(jnp.exp(logits - peak[None, :]), axis=0)
    hit = jnp.sum(jnp.where(is_target(targets), logits, 0.0), axis=0)
    return (peak + jnp.log(total)).reshape(-1, HALF), jnp.sum(hit.reshape(-1, HALF), axis=0, keepdims=True)


def put(into, part, row):
    return lax.dynamic_update_slice(into, part.reshape(-1, HALF, part.shape[1]), (row, ZERO, ZERO))


def body(query_emb, positive_list, centroids):
    x, z, y, core = (lax.axis_index(name) for name in DP_MP)
    sign = 1 - 2 * core
    width = query_emb.shape[1]

    steps = [0, -1, 1, -2, 2, -3, 3, 4]
    firsts = [((z + sign * step) & 7) * 2 for step in steps]
    firsts = firsts[:7] + [firsts[7] + core, firsts[7] + 1 - core]
    firsts = [first.astype(jnp.uint32) for first in firsts]
    own_base, x_at, cut, at_first = (z * 8 + y * 2 + core) * OWN, x.astype(jnp.uint32), core.astype(jnp.uint32), core == 0

    part, blocks = query_emb, [query_emb]
    for k in range(3):
        part = lax.ppermute(part, ("z", "c"), OPPOSITE)
        if k == 0:
            part, positive_list, own_base, x, x_at, cut, at_first, *firsts = lax.optimization_barrier(
                (part, positive_list, own_base, x, x_at, cut, at_first, *firsts)
            )
        swapped = lax.ppermute(part, "c", SWAP)
        blocks += [part, swapped]
    part = lax.dynamic_slice(part.reshape(2, HALF, width), (cut, ZERO, ZERO), (1, HALF, width))[0]
    last = lax.ppermute(part, ("z", "c"), OPPOSITE)
    swapped = lax.ppermute(last, "c", SWAP)
    blocks = list(zip(blocks + [last, swapped], firsts))

    half = centroids.astype(jnp.bfloat16)
    lists = jnp.concatenate([lax.ppermute(half, "x", turn(4, -hop)) if hop else half for hop in HOPS])
    lists = lax.optimization_barrier(lists)

    targets = lax.dynamic_slice(positive_list.reshape(4, 2048), (x_at, ZERO), (1, 2048))[0] - own_base
    place = (((targets >> 13) - x + 3) & 3) * OWN + (targets & (OWN - 1))
    targets = jnp.where((targets & 8191) < OWN, place, -1)
    late = [lax.dynamic_slice(targets.reshape(16, HALF), (row, ZERO), (block.shape[0] // HALF, HALF)) for block, row in blocks[5:]]
    targets, *late = lax.optimization_barrier((targets, *[some.reshape(-1) for some in late]))
    rows = jnp.zeros((16, HALF, width), query_emb.dtype)
    for block, row in blocks[:5]:
        rows = put(rows, block, row)
    state, hit = forward(rows.reshape(-1, width), lists, targets)
    at = lax.broadcasted_iota(jnp.uint32, (16, HALF), 0)
    for i, (block, row) in enumerate(blocks[5:]):
        local, more = forward(block, lists, late[i])
        state, hit = jnp.where(at == row, local[:1], state), hit + more
        if i < 2:
            state = jnp.where(at - 1 == row, local[1:], state)
            rows = put(rows, block, row)
    state = jnp.concatenate([state, hit, jnp.zeros((7, HALF), jnp.float32)])
    for block, row in blocks[7:]:
        rows = put(rows, block, row)
    rows = rows.reshape(-1, width)
    state = over_lists(state, at_first)

    rows, lists, log_norm = lax.optimization_barrier((rows, lists, state[:16].reshape(-1)))
    hot = is_target(targets).astype(jnp.float32)
    weights = (jnp.exp(logits_of(rows, lists) - log_norm[None, :]) - hot).astype(jnp.bfloat16)
    weights = lax.optimization_barrier(weights)
    sent = jnp.dot(weights[: 3 * OWN], rows, preferred_element_type=jnp.float32)
    sent = (sent * SCALE).astype(jnp.float16)
    back = []
    for some, step in ((slice(128, 192), 2), (slice(192, 256), -2), (slice(0, 128), 1), (slice(256, 384), -1)):
        back.append(lax.ppermute(sent[some], "x", turn(4, step)).astype(jnp.float32))
    own = jnp.dot(weights[3 * OWN :], rows, preferred_element_type=jnp.float32)
    own = lax.optimization_barrier(own)
    at = lax.broadcasted_iota(jnp.int32, state.shape, 0)
    loss = jnp.full((8, 128), jnp.sum(jnp.where(at < 16, state, -state)))
    others = []
    for step in (2, 1, -1):
        others.append(lax.ppermute(loss, "x", turn(4, step)))
    gradient = own + (jnp.concatenate(back[:2]) + back[2] + back[3]) * (1.0 / SCALE)
    return (gradient, loss + others[0] + others[1] + others[2])


def shards(query_emb, positive_list, centroids, first_moment, second_moment):
    gradient, loss = body(query_emb, positive_list, centroids)
    new_centroids, new_first, new_second = adam_update(centroids, first_moment, second_moment, gradient)
    return (new_centroids, new_first, new_second, loss[0, 0] / ROWS)


def solution(mesh):
    split = Mesh(mesh.devices.reshape(4, 8, 4, 2), DP_MP)
    placed = (P(DP, None), P(), P(DP_MP, None), P(DP_MP, None), P(DP_MP, None))
    return jax.shard_map(
        shards,
        mesh=split,
        in_specs=placed,
        out_specs=(P(DP_MP, None), P(DP_MP, None), P(DP_MP, None), P()),
        check_vma=False,
    )
```

```python
import functools

import jax
import jax.numpy as jnp
import numpy as np
from jax import lax
from jax.sharding import Mesh
from jax.sharding import PartitionSpec as P


DP = ("x", "z")
DP_MP = ("x", "z", "y", "c")

beta_first = 0.9
beta_second = 0.95
learn_rate = 0.01
epsilon = 1e-08
ROWS = 8192
HALF = 128
OWN = 128
HOPS = (1, 2, 3, 0)
ZERO = np.uint32(0)
SCALE = 4.0


def turn(size, step):
    return [(i, (i + step) % size) for i in range(size)]


SWAP = [(0, 1), (1, 0)]
OPPOSITE = [(z * 2 + c, (z + (1, -1)[c]) % 8 * 2 + c) for z in range(8) for c in range(2)]


def adam_update(centroids, first_moment, second_moment, gradient):
    new_first = beta_first * first_moment + (1.0 - beta_first) * gradient
    new_second = beta_second * second_moment + (1.0 - beta_second) * gradient * gradient
    new_centroids = centroids - learn_rate * new_first / (jnp.sqrt(new_second) + epsilon)
    return (new_centroids, new_first, new_second)


def join(*parts):
    top = functools.reduce(jnp.maximum, parts)
    joined = top + jnp.log(sum(jnp.exp(part - top) for part in parts))
    return jnp.where(lax.broadcasted_iota(jnp.int32, top.shape, 0) < 16, joined, sum(parts))


def over_lists(state, at_first):
    state = join(state, lax.ppermute(state, "c", SWAP))
    pair = join(state, lax.ppermute(state, ("z", "c"), OPPOSITE))
    some = lax.ppermute(pair, ("z", "c"), [(z * 2 + c, (z + (2, -3)[c]) % 8 * 2 + c) for z in range(8) for c in range(2)])
    rest = lax.ppermute(pair, ("z", "c"), [(z * 2 + 1, (z - 1) % 8 * 2 + 1) for z in range(8)])
    state = join(some, jnp.where(at_first, pair, rest))
    state = join(state, *[lax.ppermute(state, "y", turn(4, step)) for step in (2, 1, -1)])
    return join(state, lax.ppermute(state, "c", SWAP))


def is_target(targets):
    return lax.broadcasted_iota(jnp.int32, (4 * OWN, targets.shape[0]), 0) == targets[None, :]


def logits_of(rows, lists):
    return jnp.einsum("kd,rd->kr", lists, rows, preferred_element_type=jnp.float32)


def logits_of(rows, lists):
    return jnp.einsum("kd,rd->kr", lists, rows, preferred_element_type=jnp.float32)


def forward(rows, lists, targets):
    logits = logits_of(rows, lists)
    peak = jnp.max(logits, axis=0)
    logits, peak = lax.optimization_barrier((logits, peak))
    total = jnp.sum(jnp.exp(logits - peak[None, :]), axis=0)
    hit = jnp.sum(jnp.where(is_target(targets), logits, 0.0), axis=0)
    return (peak + jnp.log(total)).reshape(-1, HALF), jnp.sum(hit.reshape(-1, HALF), axis=0, keepdims=True)


def put(into, part, row):
    return lax.dynamic_update_slice(into, part.reshape(-1, HALF, part.shape[1]), (row, ZERO, ZERO))


def body(query_emb, positive_list, centroids):
    x, z, y, core = (lax.axis_index(name) for name in DP_MP)
    sign = 1 - 2 * core
    width = query_emb.shape[1]

    def slot(step, half):
        return ((((z + sign * step) & 7) * 2) + half).astype(jnp.uint32)

    own_at, one = slot(0, 0), [slot(-1, 0), slot(1, 0)]
    two, three = [[slot(step, half) for step, half in ((-k, core), (-k, 1 - core), (k, 1 - core), (k, core))] for k in (2, 3)]
    four = [slot(4, core), slot(4, 1 - core)]
    own_base, x_at, cut, at_first = (z * 8 + y * 2 + core) * OWN, x.astype(jnp.uint32), core.astype(jnp.uint32), core == 0

    targets = lax.dynamic_slice(positive_list.reshape(4, 2048), (x_at, ZERO), (1, 2048))[0] - own_base
    place = (((targets >> 13) - x + 3) & 3) * OWN + (targets & (OWN - 1))
    targets = jnp.where((targets & 8191) < OWN, place, -1)
    late = [lax.dynamic_slice(targets.reshape(16, HALF), (row, ZERO), (1, HALF))[0] for row in four]

    part = lax.ppermute(query_emb, ("z", "c"), OPPOSITE)
    part, own_at, one, two, three, four, cut, at_first, targets, late = lax.optimization_barrier(
        (part, own_at, one, two, three, four, cut, at_first, targets, late)
    )
    swapped = lax.ppermute(part, "c", SWAP)
    rows = jnp.zeros((16, HALF, width), query_emb.dtype)
    for block, row in zip((query_emb, part, swapped), [own_at] + one):
        rows = put(rows, block, row)
    part = part.reshape(2, HALF, width)
    parts = [lax.dynamic_slice(part, (at, ZERO, ZERO), (1, HALF, width))[0] for at in (cut, 1 - cut)]
    arrived = []
    for _ in range(2):
        for i in range(2):
            parts[i] = lax.ppermute(parts[i], ("z", "c"), OPPOSITE)
        swapped = []
        for i in range(2):
            swapped.append(lax.ppermute(parts[i], "c", SWAP))
        arrived.append(parts + swapped)
    last = lax.ppermute(parts[0], ("z", "c"), OPPOSITE)
    swapped = lax.ppermute(last, "c", SWAP)
    for block, row in zip(arrived[0] + arrived[1], two + three):
        rows = put(rows, block, row)

    half = centroids.astype(jnp.bfloat16)
    lists = jnp.concatenate([lax.ppermute(half, "x", turn(4, -hop)) if hop else half for hop in HOPS])
    lists = lax.optimization_barrier(lists)

    state, hit = forward(rows.reshape(-1, width), lists, targets)
    at = lax.broadcasted_iota(jnp.uint32, (16, HALF), 0)
    for i, (block, row) in enumerate(zip((last, swapped), four)):
        local, more = forward(block, lists, late[i])
        state, hit = jnp.where(at == row, local, state), hit + more
        rows = put(rows, block, row)
    state = jnp.concatenate([state, hit, jnp.zeros((7, HALF), jnp.float32)])
    rows = rows.reshape(-1, width)
    state = over_lists(state, at_first)

    rows, lists, log_norm = lax.optimization_barrier((rows, lists, state[:16].reshape(-1)))
    hot = is_target(targets).astype(jnp.float32)
    weights = (jnp.exp(logits_of(rows, lists) - log_norm[None, :]) - hot).astype(jnp.bfloat16)
    weights = lax.optimization_barrier(weights)
    sent = jnp.dot(weights[: 3 * OWN], rows, preferred_element_type=jnp.float32)
    sent = (sent * SCALE).astype(jnp.float16)
    back = []
    for some, step in ((slice(128, 192), 2), (slice(192, 256), -2), (slice(0, 128), 1), (slice(256, 384), -1)):
        back.append(lax.ppermute(sent[some], "x", turn(4, step)).astype(jnp.float32))
    own = jnp.dot(weights[3 * OWN :], rows, preferred_element_type=jnp.float32)
    own = lax.optimization_barrier(own)
    at = lax.broadcasted_iota(jnp.int32, state.shape, 0)
    loss = jnp.sum(jnp.where(at < 16, state, -state)).reshape(1, 1)
    others = []
    for step in (2, 1, -1):
        others.append(lax.ppermute(loss, "x", turn(4, step)))
    gradient = own + (jnp.concatenate(back[:2]) + back[2] + back[3]) * (1.0 / SCALE)
    return (gradient, [loss] + others)


def shards(query_emb, positive_list, centroids, first_moment, second_moment):
    gradient, loss = body(query_emb, positive_list, centroids)
    new_centroids, new_first, new_second = adam_update(centroids, first_moment, second_moment, gradient)
    new_first, *loss = lax.optimization_barrier((new_first, *loss))
    return (new_centroids, new_first, new_second, sum(loss).reshape(()) / ROWS)


def solution(mesh):
    split = Mesh(mesh.devices.reshape(4, 8, 4, 2), DP_MP)
    placed = (P(DP, None), P(), P(DP_MP, None), P(DP_MP, None), P(DP_MP, None))
    return jax.shard_map(
        shards,
        mesh=split,
        in_specs=placed,
        out_specs=(P(DP_MP, None), P(DP_MP, None), P(DP_MP, None), P()),
        check_vma=False,
    )
```

```python
import functools

import jax
import jax.numpy as jnp
import numpy as np
from jax import lax
from jax.sharding import Mesh
from jax.sharding import PartitionSpec as P


DP = ("x", "z")
DP_MP = ("x", "z", "y", "c")

beta_first = 0.9
beta_second = 0.95
learn_rate = 0.01
epsilon = 1e-08
ROWS = 8192
HALF = 128
OWN = 128
HOPS = (1, 2, 3, 0)
ZERO = np.uint32(0)
SCALE = 4.0


def turn(size, step):
    return [(i, (i + step) % size) for i in range(size)]


SWAP = [(0, 1), (1, 0)]
OPPOSITE = [(z * 2 + c, (z + (1, -1)[c]) % 8 * 2 + c) for z in range(8) for c in range(2)]


def after(x, *others):
    return lax.optimization_barrier((x, *others))[0]


def adam_update(centroids, first_moment, second_moment, gradient):
    new_first = beta_first * first_moment + (1.0 - beta_first) * gradient
    new_second = beta_second * second_moment + (1.0 - beta_second) * gradient * gradient
    new_centroids = centroids - learn_rate * new_first / (jnp.sqrt(new_second) + epsilon)
    return (new_centroids, new_first, new_second)


def join(*parts):
    top = functools.reduce(jnp.maximum, parts)
    joined = top + jnp.log(sum(jnp.exp(part - top) for part in parts))
    return jnp.where(lax.broadcasted_iota(jnp.int32, top.shape, 0) < 16, joined, sum(parts))


def over_lists(state, at_first):
    state = join(state, lax.ppermute(state, "c", SWAP))
    pair = join(state, lax.ppermute(state, ("z", "c"), OPPOSITE))
    some = lax.ppermute(pair, ("z", "c"), [(z * 2 + c, (z + (2, -3)[c]) % 8 * 2 + c) for z in range(8) for c in range(2)])
    rest = lax.ppermute(pair, ("z", "c"), [(z * 2 + 1, (z - 1) % 8 * 2 + 1) for z in range(8)])
    state = join(some, jnp.where(at_first, pair, rest))
    state = join(state, *[lax.ppermute(state, "y", turn(4, step)) for step in (2, 1, -1)])
    return join(state, lax.ppermute(state, "c", SWAP))


def is_target(targets):
    return lax.broadcasted_iota(jnp.int32, (4 * OWN, targets.shape[0]), 0) == targets[None, :]


def logits_of(rows, lists):
    return jnp.einsum("kd,rd->kr", lists, rows, preferred_element_type=jnp.float32)


def logits_of(rows, lists):
    return jnp.einsum("kd,rd->kr", lists, rows, preferred_element_type=jnp.float32)


def forward(rows, lists, targets):
    logits = logits_of(rows, lists)
    peak = jnp.max(logits, axis=0)
    logits, peak = lax.optimization_barrier((logits, peak))
    total = jnp.sum(jnp.exp(logits - peak[None, :]), axis=0)
    hit = jnp.sum(jnp.where(is_target(targets), logits, 0.0), axis=0)
    return (peak + jnp.log(total)).reshape(-1, HALF), jnp.sum(hit.reshape(-1, HALF), axis=0, keepdims=True)


def put(into, part, row):
    return lax.dynamic_update_slice(into, part.reshape(-1, HALF, part.shape[1]), (row, ZERO, ZERO))


def body(query_emb, positive_list, centroids):
    x, z, y, core = (lax.axis_index(name) for name in DP_MP)
    sign = 1 - 2 * core
    width = query_emb.shape[1]

    def slot(step, half):
        return ((((z + sign * step) & 7) * 2) + half).astype(jnp.uint32)

    own_at, one = slot(0, 0), [slot(-1, 0), slot(1, 0)]
    two, three = [[slot(step, half) for step, half in ((-k, core), (-k, 1 - core), (k, 1 - core), (k, core))] for k in (2, 3)]
    four = [slot(4, core), slot(4, 1 - core)]
    own_base, x_at, cut, at_first = (z * 8 + y * 2 + core) * OWN, x.astype(jnp.uint32), core.astype(jnp.uint32), core == 0

    targets = lax.dynamic_slice(positive_list.reshape(4, 2048), (x_at, ZERO), (1, 2048))[0] - own_base
    place = (((targets >> 13) - x + 3) & 3) * OWN + (targets & (OWN - 1))
    targets = jnp.where((targets & 8191) < OWN, place, -1)
    late = [lax.dynamic_slice(targets.reshape(16, HALF), (row, ZERO), (1, HALF))[0] for row in four]

    part = lax.ppermute(query_emb, ("z", "c"), OPPOSITE)
    part, own_at, one, two, three, four, cut, at_first, targets, late = lax.optimization_barrier(
        (part, own_at, one, two, three, four, cut, at_first, targets, late)
    )
    swapped = lax.ppermute(part, "c", SWAP)
    rows = jnp.zeros((16, HALF, width), query_emb.dtype)
    for block, row in zip((query_emb, part, swapped), [own_at] + one):
        rows = put(rows, block, row)
    part = part.reshape(2, HALF, width)
    parts = [lax.dynamic_slice(part, (at, ZERO, ZERO), (1, HALF, width))[0] for at in (cut, 1 - cut)]
    arrived = []
    for _ in range(2):
        for i in range(2):
            parts[i] = lax.ppermute(parts[i], ("z", "c"), OPPOSITE)
        swapped = []
        for i in range(2):
            swapped.append(lax.ppermute(parts[i], "c", SWAP))
        arrived.append(parts + swapped)
    last = lax.ppermute(parts[0], ("z", "c"), OPPOSITE)
    swapped = lax.ppermute(last, "c", SWAP)
    for block, row in zip(arrived[0] + arrived[1], two + three):
        rows = put(rows, block, row)

    half = centroids.astype(jnp.bfloat16)
    lists = jnp.concatenate([lax.ppermute(half, "x", turn(4, -hop)) if hop else half for hop in HOPS])
    lists = lax.optimization_barrier(lists)

    state, hit = forward(rows.reshape(-1, width), lists, targets)
    at = lax.broadcasted_iota(jnp.uint32, (16, HALF), 0)
    for i, (block, row) in enumerate(zip((last, swapped), four)):
        local, more = forward(block, lists, late[i])
        state, hit = jnp.where(at == row, local, state), hit + more
        rows = put(rows, block, row)
    state = jnp.concatenate([state, hit, jnp.zeros((7, HALF), jnp.float32)])
    rows = rows.reshape(-1, width)
    state = over_lists(state, at_first)

    rows, lists, log_norm = lax.optimization_barrier((rows, lists, state[:16].reshape(-1)))
    hot = is_target(targets).astype(jnp.float32)
    weights = (jnp.exp(logits_of(rows, lists) - log_norm[None, :]) - hot).astype(jnp.bfloat16)
    weights = lax.optimization_barrier(weights)
    sent = jnp.dot(weights[: 3 * OWN], rows, preferred_element_type=jnp.float32)
    sent = (sent * SCALE).astype(jnp.float16)
    back = []
    for some, step in ((slice(128, 256), 2), (slice(0, 128), 1), (slice(256, 384), -1)):
        back.append(lax.ppermute(sent[some], "x", turn(4, step)).astype(jnp.float32))
    own = jnp.dot(weights[3 * OWN :], rows, preferred_element_type=jnp.float32)
    own = lax.optimization_barrier(own)
    at = lax.broadcasted_iota(jnp.int32, state.shape, 0)
    state = after(state, sent)
    loss = jnp.sum(jnp.where(at < 16, state, -state)).reshape(1, 1)
    others = []
    for step in (2, 1, -1):
        others.append(lax.ppermute(loss, "x", turn(4, step)))
    gradient = own + (back[0] + back[1] + back[2]) * (1.0 / SCALE)
    return (gradient, [loss] + others)


def shards(query_emb, positive_list, centroids, first_moment, second_moment):
    gradient, loss = body(query_emb, positive_list, centroids)
    new_centroids, new_first, new_second = adam_update(centroids, first_moment, second_moment, gradient)
    new_first, *loss = lax.optimization_barrier((new_first, *loss))
    return (new_centroids, new_first, new_second, sum(loss).reshape(()) / ROWS)


def solution(mesh):
    split = Mesh(mesh.devices.reshape(4, 8, 4, 2), DP_MP)
    placed = (P(DP, None), P(), P(DP_MP, None), P(DP_MP, None), P(DP_MP, None))
    return jax.shard_map(
        shards,
        mesh=split,
        in_specs=placed,
        out_specs=(P(DP_MP, None), P(DP_MP, None), P(DP_MP, None), P()),
        check_vma=False,
    )
```

```python
import functools

import jax
import jax.numpy as jnp
import numpy as np
from jax import lax
from jax.sharding import Mesh
from jax.sharding import PartitionSpec as P


DP = ("x", "z")
DP_MP = ("x", "z", "y", "c")

beta_first = 0.9
beta_second = 0.95
learn_rate = 0.01
epsilon = 1e-08
ROWS = 8192
HALF = 128
OWN = 128
HOPS = (1, 2, 3, 0)
ZERO = np.uint32(0)
NOTHING = -1e30
SCALE = 4.0


def turn(size, step):
    return [(i, (i + step) % size) for i in range(size)]


SWAP = [(0, 1), (1, 0)]
OPPOSITE = [(z * 2 + c, (z + (1, -1)[c]) % 8 * 2 + c) for z in range(8) for c in range(2)]


def after(x, *others):
    return lax.optimization_barrier((x, *others))[0]


def adam_update(centroids, first_moment, second_moment, gradient):
    new_first = beta_first * first_moment + (1.0 - beta_first) * gradient
    new_second = beta_second * second_moment + (1.0 - beta_second) * gradient * gradient
    new_centroids = centroids - learn_rate * new_first / (jnp.sqrt(new_second) + epsilon)
    return (new_centroids, new_first, new_second)


def join(*parts):
    top = functools.reduce(jnp.maximum, parts)
    joined = top + jnp.log(sum(jnp.exp(part - top) for part in parts))
    return jnp.where(lax.broadcasted_iota(jnp.int32, top.shape, 0) < 16, joined, sum(parts))


def over_lists(state, at_first):
    state = join(state, lax.ppermute(state, "c", SWAP))
    pair = join(state, lax.ppermute(state, ("z", "c"), OPPOSITE))
    some = lax.ppermute(pair, ("z", "c"), [(z * 2 + c, (z + (2, -3)[c]) % 8 * 2 + c) for z in range(8) for c in range(2)])
    rest = lax.ppermute(pair, ("z", "c"), [(z * 2 + 1, (z - 1) % 8 * 2 + 1) for z in range(8)])
    state = join(some, jnp.where(at_first, pair, rest))
    state = join(state, *[lax.ppermute(state, "y", turn(4, step)) for step in (2, 1, -1)])
    return join(state, lax.ppermute(state, "c", SWAP))


def is_target(targets):
    return lax.broadcasted_iota(jnp.int32, (4 * OWN, targets.shape[0]), 0) == targets[None, :]


def logits_of(rows, lists):
    return jnp.einsum("kd,rd->kr", lists, rows, preferred_element_type=jnp.float32)


def logits_of(rows, lists):
    return jnp.einsum("kd,rd->kr", lists, rows, preferred_element_type=jnp.float32)


def forward(rows, lists, targets):
    logits = logits_of(rows, lists)
    peak = jnp.max(logits, axis=0)
    logits, peak = lax.optimization_barrier((logits, peak))
    total = jnp.sum(jnp.exp(logits - peak[None, :]), axis=0)
    hit = jnp.sum(jnp.where(is_target(targets), logits, 0.0), axis=0)
    return (peak + jnp.log(total)).reshape(-1, HALF), jnp.sum(hit.reshape(-1, HALF), axis=0, keepdims=True)


def put(into, part, row):
    return lax.dynamic_update_slice(into, part.reshape(-1, HALF, part.shape[1]), (row, ZERO, ZERO))


def body(query_emb, positive_list, centroids):
    x, z, y, core = (lax.axis_index(name) for name in DP_MP)
    sign = 1 - 2 * core
    width = query_emb.shape[1]

    def slot(step, half):
        return ((((z + sign * step) & 7) * 2) + half).astype(jnp.uint32)

    own_at, one = slot(0, 0), [slot(-1, 0), slot(1, 0)]
    two, three = [[slot(step, half) for step, half in ((-k, core), (-k, 1 - core), (k, 1 - core), (k, core))] for k in (2, 3)]
    four = [slot(4, core), slot(4, 1 - core)]
    own_base, x_at, cut, at_first = (z * 8 + y * 2 + core) * OWN, x.astype(jnp.uint32), core.astype(jnp.uint32), core == 0

    def places(base):
        some = lax.dynamic_slice(positive_list.reshape(4, 2048), (x_at, ZERO), (1, 2048))[0] - base
        place = (((some >> 13) - x + 3) & 3) * OWN + (some & (OWN - 1))
        return jnp.where((some & 8191) < OWN, place, -1)

    targets, other_targets = places(own_base), places((z * 8 + y * 2 + 1 - core) * OWN)
    mine, others = three[:2] + four[:1], three[2:] + four[1:]
    late = [
        [lax.dynamic_slice(some.reshape(16, HALF), (row, ZERO), (1, HALF))[0] for some in (targets, other_targets)]
        for row in mine
    ]

    part = lax.ppermute(query_emb, ("z", "c"), OPPOSITE)
    part, own_at, one, two, three, four, mine, others, cut, at_first, targets, late = lax.optimization_barrier(
        (part, own_at, one, two, three, four, mine, others, cut, at_first, targets, late)
    )
    swapped = lax.ppermute(part, "c", SWAP)
    rows = jnp.zeros((16, HALF, width), query_emb.dtype)
    for block, row in zip((query_emb, part, swapped), [own_at] + one):
        rows = put(rows, block, row)
    part = part.reshape(2, HALF, width)
    parts = [lax.dynamic_slice(part, (at, ZERO, ZERO), (1, HALF, width))[0] for at in (cut, 1 - cut)]
    arrived = []
    for _ in range(2):
        for i in range(2):
            parts[i] = lax.ppermute(parts[i], ("z", "c"), OPPOSITE)
        swapped = []
        for i in range(2):
            swapped.append(lax.ppermute(parts[i], "c", SWAP))
        arrived.append(parts + swapped)
    last = lax.ppermute(parts[0], ("z", "c"), OPPOSITE)
    swapped = lax.ppermute(last, "c", SWAP)
    for block, row in zip(arrived[0], two):
        rows = put(rows, block, row)

    half = centroids.astype(jnp.bfloat16)
    lists = jnp.concatenate([lax.ppermute(half, "x", turn(4, -hop)) if hop else half for hop in HOPS])
    lists = lax.optimization_barrier(lists)
    other_lists = lax.ppermute(lists, "c", SWAP)

    state, hit = forward(rows.reshape(-1, width), lists, targets)
    at = lax.broadcasted_iota(jnp.uint32, (16, HALF), 0)
    for i, (block, row) in enumerate(zip(arrived[1][:2] + [last], mine)):
        local, more = forward(block, lists, late[i][0])
        other_local, other_more = forward(block, other_lists, late[i][1])
        top = jnp.maximum(local, other_local)
        local = top + jnp.log(jnp.exp(local - top) + jnp.exp(other_local - top))
        state, hit = jnp.where(at == row, local, state), hit + more + other_more
    for row in others:
        state = jnp.where(at == row, NOTHING, state)
    for block, row in zip(arrived[1] + [last, swapped], three + four):
        rows = put(rows, block, row)
    state = jnp.concatenate([state, hit, jnp.zeros((7, HALF), jnp.float32)])
    rows = rows.reshape(-1, width)
    state = over_lists(state, at_first)

    rows, lists, log_norm = lax.optimization_barrier((rows, lists, state[:16].reshape(-1)))
    hot = is_target(targets).astype(jnp.float32)
    weights = (jnp.exp(logits_of(rows, lists) - log_norm[None, :]) - hot).astype(jnp.bfloat16)
    weights = lax.optimization_barrier(weights)
    sent = jnp.dot(weights[: 3 * OWN], rows, preferred_element_type=jnp.float32)
    sent = (sent * SCALE).astype(jnp.float16)
    back = []
    for some, step in ((slice(128, 256), 2), (slice(0, 128), 1), (slice(256, 384), -1)):
        back.append(lax.ppermute(sent[some], "x", turn(4, step)).astype(jnp.float32))
    own = jnp.dot(weights[3 * OWN :], rows, preferred_element_type=jnp.float32)
    own = lax.optimization_barrier(own)
    at = lax.broadcasted_iota(jnp.int32, state.shape, 0)
    state = after(state, sent)
    loss = jnp.sum(jnp.where(at < 16, state, -state)).reshape(1, 1)
    others = []
    for step in (2, 1, -1):
        others.append(lax.ppermute(loss, "x", turn(4, step)))
    gradient = own + (back[0] + back[1] + back[2]) * (1.0 / SCALE)
    return (gradient, [loss] + others)


def shards(query_emb, positive_list, centroids, first_moment, second_moment):
    gradient, loss = body(query_emb, positive_list, centroids)
    new_centroids, new_first, new_second = adam_update(centroids, first_moment, second_moment, gradient)
    new_first, *loss = lax.optimization_barrier((new_first, *loss))
    return (new_centroids, new_first, new_second, sum(loss).reshape(()) / ROWS)


def solution(mesh):
    split = Mesh(mesh.devices.reshape(4, 8, 4, 2), DP_MP)
    placed = (P(DP, None), P(), P(DP_MP, None), P(DP_MP, None), P(DP_MP, None))
    return jax.shard_map(
        shards,
        mesh=split,
        in_specs=placed,
        out_specs=(P(DP_MP, None), P(DP_MP, None), P(DP_MP, None), P()),
        check_vma=False,
    )
```

```python
import functools

import jax
import jax.numpy as jnp
import numpy as np
from jax import lax
from jax.sharding import Mesh
from jax.sharding import PartitionSpec as P


DP = ("x", "z")
DP_MP = ("x", "z", "y", "c")

beta_first = 0.9
beta_second = 0.95
learn_rate = 0.01
epsilon = 1e-08
ROWS = 8192
HALF = 128
OWN = 128
HOPS = (1, 2, 3, 0)
ZERO = np.uint32(0)
NOTHING = -1e30
SCALE = 4.0


def turn(size, step):
    return [(i, (i + step) % size) for i in range(size)]


SWAP = [(0, 1), (1, 0)]
OPPOSITE = [(z * 2 + c, (z + (1, -1)[c]) % 8 * 2 + c) for z in range(8) for c in range(2)]


def after(x, *others):
    return lax.optimization_barrier((x, *others))[0]


def adam_update(centroids, first_moment, second_moment, gradient):
    new_first = beta_first * first_moment + (1.0 - beta_first) * gradient
    new_second = beta_second * second_moment + (1.0 - beta_second) * gradient * gradient
    new_centroids = centroids - learn_rate * new_first / (jnp.sqrt(new_second) + epsilon)
    return (new_centroids, new_first, new_second)


def join(*parts):
    top = functools.reduce(jnp.maximum, parts)
    joined = top + jnp.log(sum(jnp.exp(part - top) for part in parts))
    return jnp.where(lax.broadcasted_iota(jnp.int32, top.shape, 0) < 16, joined, sum(parts))


def over_lists(state, at_first):
    state = join(state, lax.ppermute(state, "c", SWAP))
    pair = join(state, lax.ppermute(state, ("z", "c"), OPPOSITE))
    some = lax.ppermute(pair, ("z", "c"), [(z * 2 + c, (z + (2, -3)[c]) % 8 * 2 + c) for z in range(8) for c in range(2)])
    rest = lax.ppermute(pair, ("z", "c"), [(z * 2 + 1, (z - 1) % 8 * 2 + 1) for z in range(8)])
    state = join(some, jnp.where(at_first, pair, rest))
    state = join(state, *[lax.ppermute(state, "y", turn(4, step)) for step in (2, 1, -1)])
    return join(state, lax.ppermute(state, "c", SWAP))


def is_target(targets):
    return lax.broadcasted_iota(jnp.int32, (4 * OWN, targets.shape[0]), 0) == targets[None, :]


def logits_of(rows, lists):
    return jnp.einsum("kd,rd->kr", lists, rows, preferred_element_type=jnp.float32)


def logits_of(rows, lists):
    return jnp.einsum("kd,rd->kr", lists, rows, preferred_element_type=jnp.float32)


def forward(rows, lists, targets):
    logits = logits_of(rows, lists)
    peak = jnp.max(logits, axis=0)
    logits, peak = lax.optimization_barrier((logits, peak))
    total = jnp.sum(jnp.exp(logits - peak[None, :]), axis=0)
    hit = jnp.sum(jnp.where(is_target(targets), logits, 0.0), axis=0)
    return (peak + jnp.log(total)).reshape(-1, HALF), jnp.sum(hit.reshape(-1, HALF), axis=0, keepdims=True)


def put(into, part, row):
    return lax.dynamic_update_slice(into, part.reshape(-1, HALF, part.shape[1]), (row, ZERO, ZERO))


def body(query_emb, positive_list, centroids):
    x, z, y, core = (lax.axis_index(name) for name in DP_MP)
    sign = 1 - 2 * core
    width = query_emb.shape[1]

    def slot(step, half):
        return ((((z + sign * step) & 7) * 2) + half).astype(jnp.uint32)

    own_at = slot(0, 0)
    one, two, three = [
        [slot(step, half) for step, half in ((-k, core), (-k, 1 - core), (k, 1 - core), (k, core))] for k in (1, 2, 3)
    ]
    four = [slot(4, core), slot(4, 1 - core)]
    own_base, x_at, cut, at_first = (z * 8 + y * 2 + core) * OWN, x.astype(jnp.uint32), core.astype(jnp.uint32), core == 0

    def places(base):
        some = lax.dynamic_slice(positive_list.reshape(4, 2048), (x_at, ZERO), (1, 2048))[0] - base
        place = (((some >> 13) - x + 3) & 3) * OWN + (some & (OWN - 1))
        return jnp.where((some & 8191) < OWN, place, -1)

    targets, other_targets = places(own_base), places((z * 8 + y * 2 + 1 - core) * OWN)
    mine, others = three[:2] + four[:1], three[2:] + four[1:]
    late = [
        [lax.dynamic_slice(some.reshape(16, HALF), (row, ZERO), (1, HALF))[0] for some in (targets, other_targets)]
        for row in mine
    ]

    parts = [lax.dynamic_slice(query_emb.reshape(2, HALF, width), (at, ZERO, ZERO), (1, HALF, width))[0] for at in (cut, 1 - cut)]
    for i in range(2):
        parts[i] = lax.ppermute(parts[i], ("z", "c"), OPPOSITE)
    parts[0], own_at, one, two, three, four, mine, others, at_first = lax.optimization_barrier(
        (parts[0], own_at, one, two, three, four, mine, others, at_first)
    )
    swapped = []
    for i in range(2):
        swapped.append(lax.ppermute(parts[i], "c", SWAP))
    rows = jnp.zeros((16, HALF, width), query_emb.dtype)
    rows = put(rows, query_emb, own_at)
    for block, row in zip(parts + swapped, one):
        rows = put(rows, block, row)
    arrived = []
    for _ in range(2):
        for i in range(2):
            parts[i] = lax.ppermute(parts[i], ("z", "c"), OPPOSITE)
        swapped = []
        for i in range(2):
            swapped.append(lax.ppermute(parts[i], "c", SWAP))
        arrived.append(parts + swapped)
    last = lax.ppermute(parts[0], ("z", "c"), OPPOSITE)
    swapped = lax.ppermute(last, "c", SWAP)
    for block, row in zip(arrived[0], two):
        rows = put(rows, block, row)

    half = centroids.astype(jnp.bfloat16)
    lists = []
    for hop in HOPS[:3]:
        lists.append(lax.ppermute(half, "x", turn(4, -hop)))
    lists = jnp.concatenate(lists + [half])
    lists = lax.optimization_barrier(lists)
    other_lists = lax.ppermute(lists, "c", SWAP)

    state, hit = forward(rows.reshape(-1, width), lists, targets)
    at = lax.broadcasted_iota(jnp.uint32, (16, HALF), 0)
    for i, (block, row) in enumerate(zip(arrived[1][:2] + [last], mine)):
        local, more = forward(block, lists, late[i][0])
        other_local, other_more = forward(block, other_lists, late[i][1])
        top = jnp.maximum(local, other_local)
        local = top + jnp.log(jnp.exp(local - top) + jnp.exp(other_local - top))
        state, hit = jnp.where(at == row, local, state), hit + more + other_more
    for row in others:
        state = jnp.where(at == row, NOTHING, state)
    for block, row in zip(arrived[1] + [last, swapped], three + four):
        rows = put(rows, block, row)
    state = jnp.concatenate([state, hit, jnp.zeros((7, HALF), jnp.float32)])
    rows = rows.reshape(-1, width)
    state = over_lists(state, at_first)

    rows, lists, log_norm = lax.optimization_barrier((rows, lists, state[:16].reshape(-1)))
    hot = is_target(targets).astype(jnp.float32)
    weights = (jnp.exp(logits_of(rows, lists) - log_norm[None, :]) - hot).astype(jnp.bfloat16)
    weights = lax.optimization_barrier(weights)
    sent = jnp.dot(weights[: 3 * OWN], rows, preferred_element_type=jnp.float32)
    sent = (sent * SCALE).astype(jnp.float16)
    back = []
    for some, step in ((slice(128, 256), 2), (slice(0, 128), 1), (slice(256, 384), -1)):
        back.append(lax.ppermute(sent[some], "x", turn(4, step)).astype(jnp.float32))
    own = jnp.dot(weights[3 * OWN :], rows, preferred_element_type=jnp.float32)
    own = lax.optimization_barrier(own)
    at = lax.broadcasted_iota(jnp.int32, state.shape, 0)
    state = after(state, sent)
    loss = jnp.sum(jnp.where(at < 16, state, -state)).reshape(1, 1)
    others = []
    for step in (2, 1, -1):
        others.append(lax.ppermute(loss, "x", turn(4, step)))
    gradient = own + (back[0] + back[1] + back[2]) * (1.0 / SCALE)
    return (gradient, [loss] + others)


def shards(query_emb, positive_list, centroids, first_moment, second_moment):
    gradient, loss = body(query_emb, positive_list, centroids)
    new_centroids, new_first, new_second = adam_update(centroids, first_moment, second_moment, gradient)
    new_first, *loss = lax.optimization_barrier((new_first, *loss))
    return (new_centroids, new_first, new_second, sum(loss).reshape(()) / ROWS)


def solution(mesh):
    split = Mesh(mesh.devices.reshape(4, 8, 4, 2), DP_MP)
    placed = (P(DP, None), P(), P(DP_MP, None), P(DP_MP, None), P(DP_MP, None))
    return jax.shard_map(
        shards,
        mesh=split,
        in_specs=placed,
        out_specs=(P(DP_MP, None), P(DP_MP, None), P(DP_MP, None), P()),
        check_vma=False,
    )
```

```python
import functools

import jax
import jax.numpy as jnp
import numpy as np
from jax import lax
from jax.sharding import Mesh
from jax.sharding import PartitionSpec as P


DP = ("x", "z")
DP_MP = ("x", "z", "y", "c")

beta_first = 0.9
beta_second = 0.95
learn_rate = 0.01
epsilon = 1e-08
ROWS = 8192
HALF = 128
OWN = 128
HOPS = (1, 2, 3, 0)
ZERO = np.uint32(0)
NOTHING = -1e30
SCALE = 4.0


def turn(size, step):
    return [(i, (i + step) % size) for i in range(size)]


SWAP = [(0, 1), (1, 0)]
OPPOSITE = [(z * 2 + c, (z + (1, -1)[c]) % 8 * 2 + c) for z in range(8) for c in range(2)]


def after(x, *others):
    return lax.optimization_barrier((x, *others))[0]


def adam_update(centroids, first_moment, second_moment, gradient):
    new_first = beta_first * first_moment + (1.0 - beta_first) * gradient
    new_second = beta_second * second_moment + (1.0 - beta_second) * gradient * gradient
    new_centroids = centroids - learn_rate * new_first / (jnp.sqrt(new_second) + epsilon)
    return (new_centroids, new_first, new_second)


def join(*parts):
    top = functools.reduce(jnp.maximum, parts)
    joined = top + jnp.log(sum(jnp.exp(part - top) for part in parts))
    return jnp.where(lax.broadcasted_iota(jnp.int32, top.shape, 0) < 16, joined, sum(parts))


def over_lists(state, at_first):
    state = join(state, lax.ppermute(state, "c", SWAP))
    pair = join(state, lax.ppermute(state, ("z", "c"), OPPOSITE))
    some = lax.ppermute(pair, ("z", "c"), [(z * 2 + c, (z + (2, -3)[c]) % 8 * 2 + c) for z in range(8) for c in range(2)])
    rest = lax.ppermute(pair, ("z", "c"), [(z * 2 + 1, (z - 1) % 8 * 2 + 1) for z in range(8)])
    state = join(some, jnp.where(at_first, pair, rest))
    state = join(state, *[lax.ppermute(state, "y", turn(4, step)) for step in (2, 1, -1)])
    return join(state, lax.ppermute(state, "c", SWAP))


def is_target(targets):
    return lax.broadcasted_iota(jnp.int32, (4 * OWN, targets.shape[0]), 0) == targets[None, :]


def logits_of(rows, lists):
    return jnp.einsum("kd,rd->kr", lists, rows, preferred_element_type=jnp.float32)


def logits_of(rows, lists):
    return jnp.einsum("kd,rd->kr", lists, rows, preferred_element_type=jnp.float32)


def forward(rows, lists, targets):
    logits = logits_of(rows, lists)
    peak = jnp.max(logits, axis=0)
    logits, peak = lax.optimization_barrier((logits, peak))
    total = jnp.sum(jnp.exp(logits - peak[None, :]), axis=0)
    hit = jnp.sum(jnp.where(is_target(targets), logits, 0.0), axis=0)
    return (peak + jnp.log(total)).reshape(-1, HALF), jnp.sum(hit.reshape(-1, HALF), axis=0, keepdims=True)


def put(into, part, row):
    return lax.dynamic_update_slice(into, part.reshape(-1, HALF, part.shape[1]), (row, ZERO, ZERO))


def body(query_emb, positive_list, centroids):
    x, z, y, core = (lax.axis_index(name) for name in DP_MP)
    sign = 1 - 2 * core
    width = query_emb.shape[1]

    def slot(step, half):
        return ((((z + sign * step) & 7) * 2) + half).astype(jnp.uint32)

    own_at = slot(0, 0)
    one, two, three = [
        [slot(step, half) for step, half in ((-k, core), (-k, 1 - core), (k, 1 - core), (k, core))] for k in (1, 2, 3)
    ]
    four = [slot(4, core), slot(4, 1 - core)]
    own_base, x_at, cut, at_first = (z * 8 + y * 2 + core) * OWN, x.astype(jnp.uint32), core.astype(jnp.uint32), core == 0

    def places(base):
        some = lax.dynamic_slice(positive_list.reshape(4, 2048), (x_at, ZERO), (1, 2048))[0] - base
        place = (((some >> 13) - x + 3) & 3) * OWN + (some & (OWN - 1))
        return jnp.where((some & 8191) < OWN, place, -1)

    targets, other_targets = places(own_base), places((z * 8 + y * 2 + 1 - core) * OWN)
    mine, others = three[:2] + four[:1], three[2:] + four[1:]
    late = [
        [lax.dynamic_slice(some.reshape(16, HALF), (row, ZERO), (1, HALF))[0] for some in (targets, other_targets)]
        for row in mine
    ]

    parts = [lax.dynamic_slice(query_emb.reshape(2, HALF, width), (at, ZERO, ZERO), (1, HALF, width))[0] for at in (cut, 1 - cut)]
    for i in range(2):
        parts[i] = lax.ppermute(parts[i], ("z", "c"), OPPOSITE)
    parts[0], own_at, one, two, three, four, mine, others, at_first = lax.optimization_barrier(
        (parts[0], own_at, one, two, three, four, mine, others, at_first)
    )
    swapped = []
    for i in range(2):
        swapped.append(lax.ppermute(parts[i], "c", SWAP))
    rows = jnp.zeros((16, HALF, width), query_emb.dtype)
    rows = put(rows, query_emb, own_at)
    for block, row in zip(parts + swapped, one):
        rows = put(rows, block, row)
    arrived = []
    for _ in range(2):
        for i in range(2):
            parts[i] = lax.ppermute(parts[i], ("z", "c"), OPPOSITE)
        swapped = []
        for i in range(2):
            swapped.append(lax.ppermute(parts[i], "c", SWAP))
        arrived.append(parts + swapped)
    last = lax.ppermute(parts[0], ("z", "c"), OPPOSITE)
    swapped = lax.ppermute(last, "c", SWAP)
    for block, row in zip(arrived[0], two):
        rows = put(rows, block, row)

    half = centroids.astype(jnp.bfloat16)
    lists = []
    for hop in HOPS[:3]:
        lists.append(lax.ppermute(half, "x", turn(4, -hop)))
    lists = jnp.concatenate(lists + [half])
    lists = lax.optimization_barrier(lists)
    other_lists = lax.ppermute(lists, "c", SWAP)

    state, hit = forward(rows.reshape(-1, width), lists, targets)
    at = lax.broadcasted_iota(jnp.uint32, (16, HALF), 0)
    for i, (block, row) in enumerate(zip(arrived[1][:2] + [last], mine)):
        local, more = forward(block, lists, late[i][0])
        other_local, other_more = forward(block, other_lists, late[i][1])
        top = jnp.maximum(local, other_local)
        local = top + jnp.log(jnp.exp(local - top) + jnp.exp(other_local - top))
        state, hit = jnp.where(at == row, local, state), hit + more + other_more
    for row in others:
        state = jnp.where(at == row, NOTHING, state)
    for block, row in zip(arrived[1] + [last, swapped], three + four):
        rows = put(rows, block, row)
    state = jnp.concatenate([state, hit, jnp.zeros((7, HALF), jnp.float32)])
    rows = rows.reshape(-1, width)
    logits = lax.optimization_barrier(logits_of(rows, lists))
    state = over_lists(state, at_first)

    rows, log_norm = lax.optimization_barrier((rows, state[:16].reshape(-1)))
    hot = is_target(targets).astype(jnp.float32)
    weights = (jnp.exp(logits - log_norm[None, :]) - hot).astype(jnp.bfloat16)
    weights = lax.optimization_barrier(weights)
    sent = jnp.dot(weights[: 3 * OWN], rows, preferred_element_type=jnp.float32)
    sent = (sent * SCALE).astype(jnp.float16)
    back = []
    for some, step in ((slice(128, 256), 2), (slice(0, 128), 1), (slice(256, 384), -1)):
        back.append(lax.ppermute(sent[some], "x", turn(4, step)).astype(jnp.float32))
    own = jnp.dot(weights[3 * OWN :], rows, preferred_element_type=jnp.float32)
    own = lax.optimization_barrier(own)
    at = lax.broadcasted_iota(jnp.int32, state.shape, 0)
    state = after(state, sent)
    loss = jnp.sum(jnp.where(at < 16, state, -state)).reshape(1, 1)
    others = []
    for step in (2, 1, -1):
        others.append(lax.ppermute(loss, "x", turn(4, step)))
    gradient = own + (back[0] + back[1] + back[2]) * (1.0 / SCALE)
    return (gradient, [loss] + others)


def shards(query_emb, positive_list, centroids, first_moment, second_moment):
    gradient, loss = body(query_emb, positive_list, centroids)
    new_centroids, new_first, new_second = adam_update(centroids, first_moment, second_moment, gradient)
    new_first, *loss = lax.optimization_barrier((new_first, *loss))
    return (new_centroids, new_first, new_second, sum(loss).reshape(()) / ROWS)


def solution(mesh):
    split = Mesh(mesh.devices.reshape(4, 8, 4, 2), DP_MP)
    placed = (P(DP, None), P(), P(DP_MP, None), P(DP_MP, None), P(DP_MP, None))
    return jax.shard_map(
        shards,
        mesh=split,
        in_specs=placed,
        out_specs=(P(DP_MP, None), P(DP_MP, None), P(DP_MP, None), P()),
        check_vma=False,
    )
```
